128 devices in a mesh: frame: 8 (over x, core), seq: 16 (over y, z).
Axes of the slice: x: 4, y: 4, z: 4, core: 2. Of those that a mesh axis runs over, the one named last changes fastest.
Arguments:
- vit_states: bfloat16 [256, 256, 1280], P(('frame', 'seq')), may hold values from -6 to 6
- frame_slot: int32 [128], replicated, may hold values from 0 to 255, as said below
- patch_count: int32 [128], replicated, may hold values from 208 to 256, as said below
- vis_start: int32 [128], replicated, may hold values from 0 to 16383, as said below
- text_embed: bfloat16 [128, 128, 4096], P(None, ('frame', 'seq')), may hold values from -6 to 6
- vit_ln_gain: float32 [1280], replicated, may hold values from 0.25 to 1.75
- vit_ln_bias: float32 [1280], replicated, may hold values from -1.5 to 1.5
- vit_qkv_w: bfloat16 [1280, 3840], P('seq'), may hold values from -0.15625 to 0.15625
- vit_qkv_b: float32 [3840], replicated, may hold values from -1.5 to 1.5
- vit_out_w: bfloat16 [1280, 1280], P('seq'), may hold values from -0.15625 to 0.15625
- vit_out_b: float32 [1280], replicated, may hold values from -1.5 to 1.5
- proj_w: bfloat16 [1280, 4096], replicated, may hold values from -0.15625 to 0.15625
- proj_b: float32 [4096], replicated, may hold values from -1.5 to 1.5
- attn_gain: float32 [4096], replicated, may hold values from 0.25 to 1.75
- wq: bfloat16 [4096, 2048], P(None, 'frame'), may hold values from -0.09375 to 0.09375
- wk: bfloat16 [4096, 1024], P(None, 'frame'), may hold values from -0.09375 to 0.09375
- wv: bfloat16 [4096, 1024], P(None, 'frame'), may hold values from -0.09375 to 0.09375
- wo: bfloat16 [2048, 4096], P('frame'), may hold values from -0.125 to 0.125
Outputs:
- mixed: bfloat16 [128, 128, 4096], P(None, ('frame', 'seq'))
The draws below stay inside these ranges and needn't reach their ends.
Inputs may be any that keep to these rules, and one draw needn't show every extreme that they name: Frame t sits in slot frame_slot[t]; slot k of the device with index d (axes frame then seq) is d * 2 + k; no slot holds two frames. The two devices with frame indices 2i and 2i+1 and the same seq index hold exactly two frames between them; some device holds 2 frames. `patch_count`: A multiple of 4; some frame has 256 patches. Frame t's patch_count[t] / 4 visual positions start at vis_start[t] and lie within positions t * 128 to (t + 1) * 128 - 1.
All inputs are finite; a program needn't handle non-finite values.
Results may differ from the reference program's by a relative error of at most 0.015.
Values may be sent and summed in bfloat16 or wider, within the bound.
No kernel may reach another device: no remote copies, remote signals or barrier semaphores. Data moves between devices by JAX's collectives and lax.ppermute only.
A program may use at most 128 MiB of HBM per device.

```python
import math
import jax
import jax.numpy as jnp
from jax import lax

VW = 1280
VHEADS = 16
MODEL_WIDTH = 4096
QUERY_HEADS_HALF = 16
KEY_VALUE_HEADS = 8
HEAD_WIDTH = 128
FRAME_MAX = 256
SLOTS = 2
TOK_OWN = 128
VIS_MAX = 64
N_FRAME = 8
N_SEQ = 16
DEVICES = 128


def frame_spans(key):
    inner_key = jax.random.fold_in(key, 5)
    count_key, place_key = jax.random.split(inner_key)
    lowest = VIS_MAX - VIS_MAX // 5
    tokens = jax.random.randint(count_key, (DEVICES,), lowest, VIS_MAX + 1).astype(jnp.int32)
    tokens = tokens.at[0].set(VIS_MAX)
    spare = TOK_OWN - tokens
    offsets = jax.random.randint(place_key, (DEVICES,), 0, spare + 1).astype(jnp.int32)
    starts = jnp.arange(DEVICES).astype(jnp.int32) * TOK_OWN + offsets
    return (tokens * 4, starts)


def draw_patch_count(key, part):
    counts, starts = frame_spans(key)
    return counts


def draw_vis_start(key, part):
    counts, starts = frame_spans(key)
    return starts


def draw_frame_slot(key, part):
    pairs_n = DEVICES // 2
    order_key, slot_key = jax.random.split(jax.random.fold_in(key, 3))
    frames_perm = jax.random.permutation(order_key, DEVICES).astype(jnp.int32)
    scores = jax.random.randint(slot_key, (pairs_n, 4), 0, 1 << 20) * 4 + jnp.arange(4).astype(jnp.int32)[None, :]
    chosen = jnp.argsort(scores, axis=1)[:, :2].astype(jnp.int32)
    chosen = chosen.at[0].set(jnp.array([0, 1], jnp.int32))
    earlier_slot = jnp.min(chosen, axis=1)
    later_slot = jnp.max(chosen, axis=1)
    pair_ids = jnp.arange(pairs_n).astype(jnp.int32)
    low_device = pair_ids // N_SEQ * 2 * N_SEQ + pair_ids % N_SEQ
    first_slots = (low_device + earlier_slot // 2 * N_SEQ) * 2 + earlier_slot % 2
    second_slots = (low_device + later_slot // 2 * N_SEQ) * 2 + later_slot % 2
    result = jnp.zeros((DEVICES,), jnp.int32)
    result = result.at[frames_perm[0::2]].set(first_slots)
    result = result.at[frames_perm[1::2]].set(second_slots)
    return result


def level_of(own_key, dims, shards, smallest, largest):
    def one(position, shards_of):
        steps = jax.random.uniform(jax.random.fold_in(jax.random.fold_in(own_key, 6), position), (shards_of,), jnp.float32, smallest / len(shards), largest / len(shards))
        return jnp.repeat(jnp.exp(steps), dims[position] // shards_of).reshape((-1,) + (1,) * (len(dims) - position - 1))

    gain = one(*shards[0])
    for cut in shards[1:]:
        gain = gain * one(*cut)
    return gain


def normal_values(stream_key, extent, scale, limit, cuts=(), held_as=jnp.bfloat16):
    values = jax.random.normal(stream_key, extent, jnp.float32) * scale
    if len(cuts) > 0:
        values = level_of(stream_key, extent, cuts, -0.22, 0.18) * values
    return jnp.clip(values, min=-limit, max=limit).astype(held_as)


def setup_inputs(seed: int = 0) -> dict:
    key_list = jax.random.split(jax.random.key(seed), 19)
    return {
        "vit_states": normal_values(key_list[0], (DEVICES * SLOTS, FRAME_MAX, VW), 1.0, 6.0, ((0, 128),)),
        "frame_slot": draw_frame_slot(jax.random.fold_in(key_list[18], 71), 0),
        "patch_count": draw_patch_count(jax.random.fold_in(key_list[18], 71), 0),
        "vis_start": draw_vis_start(jax.random.fold_in(key_list[18], 71), 0),
        "text_embed": normal_values(key_list[4], (TOK_OWN, DEVICES, MODEL_WIDTH), 1.0, 6.0, ((1, 128),)),
        "vit_ln_gain": jnp.clip(1.0 + 0.15 * jax.random.normal(key_list[5], (VW,), jnp.float32), 0.25, 1.75),
        "vit_ln_bias": normal_values(key_list[6], (VW,), 0.3, 1.5, (), jnp.float32),
        "vit_qkv_w": normal_values(key_list[7], (VW, 3 * VW), VW ** -0.5, 0.15625, ((0, 16),)),
        "vit_qkv_b": normal_values(key_list[8], (3 * VW,), 0.3, 1.5, (), jnp.float32),
        "vit_out_w": normal_values(key_list[9], (VW, VW), VW ** -0.5, 0.15625, ((0, 16),)),
        "vit_out_b": normal_values(key_list[10], (VW,), 0.3, 1.5, (), jnp.float32),
        "proj_w": normal_values(key_list[11], (VW, MODEL_WIDTH), VW ** -0.5, 0.15625),
        "proj_b": normal_values(key_list[12], (MODEL_WIDTH,), 0.3, 1.5, (), jnp.float32),
        "attn_gain": jnp.clip(1.0 + 0.15 * jax.random.normal(key_list[13], (MODEL_WIDTH,), jnp.float32), 0.25, 1.75),
        "wq": normal_values(key_list[14], (MODEL_WIDTH, QUERY_HEADS_HALF * HEAD_WIDTH), MODEL_WIDTH ** -0.5, 0.09375, ((1, 8),)),
        "wk": normal_values(key_list[15], (MODEL_WIDTH, KEY_VALUE_HEADS * HEAD_WIDTH), MODEL_WIDTH ** -0.5, 0.09375, ((1, 8),)),
        "wv": normal_values(key_list[16], (MODEL_WIDTH, KEY_VALUE_HEADS * HEAD_WIDTH), MODEL_WIDTH ** -0.5, 0.09375, ((1, 8),)),
        "wo": normal_values(key_list[17], (QUERY_HEADS_HALF * HEAD_WIDTH, MODEL_WIDTH), (QUERY_HEADS_HALF * HEAD_WIDTH) ** -0.5, 0.125, ((0, 8),)),
    }


rope_theta = 500000.0
vit_epsilon = 1e-06
norm_epsilon = 1e-05
masked_score = -1e+30

def apply_rotary(values, rotary_angles):
    half_width = values.shape[-1] // 2
    first_half = values[..., :half_width]
    second_half = values[..., half_width:]
    cosine = jnp.cos(rotary_angles)
    sine_part = jnp.sin(rotary_angles)
    return jnp.concatenate([first_half * cosine - second_half * sine_part, second_half * cosine + first_half * sine_part], axis=-1)

def rope_angles(positions, head_size):
    exponents = jnp.arange(0, head_size, 2).astype(jnp.float32) / head_size
    inverse = jnp.power(jnp.float32(rope_theta), -exponents)
    return positions.astype(jnp.float32)[:, None] * inverse[None, :]

def vit_frame(states, patches, ln_gain, ln_bias, qkv_weight, qkv_bias, out_weight, out_bias):
    frame_max = states.shape[0]
    width_vit = states.shape[1]
    states_wide = states.astype(jnp.float32)
    average = lax.optimization_barrier(jnp.mean(states_wide, axis=1, keepdims=True))
    centred = states_wide - average
    spread = lax.optimization_barrier(jnp.mean(centred * centred, axis=1, keepdims=True))
    normed_states = (centred * lax.rsqrt(spread + vit_epsilon) * ln_gain + ln_bias).astype(jnp.bfloat16)
    projected = (jnp.dot(normed_states, qkv_weight, preferred_element_type=jnp.float32) + qkv_bias).astype(jnp.bfloat16)
    head_size = width_vit // VHEADS
    shaped = projected.reshape(frame_max, 3, VHEADS, head_size).astype(jnp.float32)
    scores = jnp.einsum('qhd,khd->hqk', shaped[:, 0], shaped[:, 1]) / math.sqrt(head_size)
    key_live = jnp.arange(frame_max).astype(jnp.int32) < patches
    scores = jnp.where(key_live[None, None, :], scores, masked_score)
    highest = lax.optimization_barrier(jnp.max(scores, axis=-1, keepdims=True))
    weights = jnp.exp(scores - highest)
    probabilities = (weights / lax.optimization_barrier(jnp.sum(weights, axis=-1, keepdims=True))).astype(jnp.bfloat16)
    context = jnp.einsum('hqk,khd->qhd', probabilities.astype(jnp.float32), shaped[:, 2]).astype(jnp.bfloat16)
    attended = jnp.dot(context.reshape(frame_max, width_vit), out_weight, preferred_element_type=jnp.float32)
    hidden = (states_wide + attended + out_bias).astype(jnp.bfloat16)
    return lax.optimization_barrier(jnp.mean(hidden.astype(jnp.float32).reshape(frame_max // 4, 4, width_vit), axis=1)).astype(jnp.bfloat16)

def reference(vit_states, frame_slot, patch_count, vis_start, text_embed, vit_ln_gain, vit_ln_bias, vit_qkv_w, vit_qkv_b, vit_out_w, vit_out_b, proj_w, proj_b, attn_gain, wq, wk, wv, wo):
    frame_states = vit_states[frame_slot]

    def encode(operands):
        states, patches = operands
        pooled = vit_frame(states, patches, vit_ln_gain, vit_ln_bias, vit_qkv_w, vit_qkv_b, vit_out_w, vit_out_b)
        return (jnp.dot(pooled, proj_w, preferred_element_type=jnp.float32) + proj_b).astype(jnp.bfloat16)
    visual = lax.map(encode, (frame_states, patch_count))
    sequence_length = TOK_OWN * DEVICES
    positions = jnp.arange(sequence_length).astype(jnp.int32)
    token_frame = positions // TOK_OWN
    within = positions - vis_start[token_frame]
    is_visual = (within >= 0) & (within < patch_count[token_frame] // 4)
    within_clip = jnp.clip(within, 0, VIS_MAX - 1)
    visual_rows = visual[token_frame, within_clip]
    merged = jnp.where(is_visual[:, None], visual_rows, text_embed.reshape(sequence_length, MODEL_WIDTH))
    merged_wide = merged.astype(jnp.float32)
    normed_states = (merged_wide * lax.rsqrt(lax.optimization_barrier(jnp.mean(merged_wide * merged_wide, axis=1, keepdims=True)) + norm_epsilon) * attn_gain).astype(jnp.bfloat16)
    rotary_angles = rope_angles(positions, HEAD_WIDTH)[:, None, :]
    query_matrix = apply_rotary(jnp.dot(normed_states, wq, preferred_element_type=jnp.float32).reshape(sequence_length, QUERY_HEADS_HALF, HEAD_WIDTH), rotary_angles).astype(jnp.bfloat16)
    keys_complete = apply_rotary(jnp.dot(normed_states, wk, preferred_element_type=jnp.float32).reshape(sequence_length, KEY_VALUE_HEADS, HEAD_WIDTH), rotary_angles).astype(jnp.bfloat16)
    values_complete = jnp.dot(normed_states, wv, preferred_element_type=jnp.float32).astype(jnp.bfloat16).reshape(sequence_length, KEY_VALUE_HEADS, HEAD_WIDTH)
    keys_wide = keys_complete.astype(jnp.float32)
    values_wide = values_complete.astype(jnp.float32)
    grouped_rows = query_matrix.reshape(sequence_length, KEY_VALUE_HEADS, QUERY_HEADS_HALF // KEY_VALUE_HEADS, HEAD_WIDTH)
    query_rows = 128

    def attend(block_index):
        offset = block_index * query_rows
        query_block = lax.dynamic_slice_in_dim(grouped_rows, offset, query_rows, 0).astype(jnp.float32)
        scores = jnp.einsum('qkgd,nkd->kgqn', query_block, keys_wide) / math.sqrt(HEAD_WIDTH)
        query_positions = offset + jnp.arange(query_rows).astype(jnp.int32)
        allowed = positions[None, :] <= query_positions[:, None]
        scores = jnp.where(allowed[None, None], scores, masked_score)
        highest = lax.optimization_barrier(jnp.max(scores, axis=-1, keepdims=True))
        weights = jnp.where(allowed[None, None], jnp.exp(scores - highest), 0.0)
        denominator = lax.optimization_barrier(jnp.sum(weights, axis=-1))
        numerator = jnp.einsum('kgqn,nkd->kgqd', weights.astype(jnp.bfloat16).astype(jnp.float32), values_wide)
        context_block = (numerator / denominator[..., None]).astype(jnp.bfloat16)
        return jnp.transpose(context_block, (2, 0, 1, 3)).reshape(query_rows, QUERY_HEADS_HALF * HEAD_WIDTH)
    context = lax.map(attend, jnp.arange(sequence_length // query_rows).astype(jnp.int32)).reshape(sequence_length, QUERY_HEADS_HALF * HEAD_WIDTH)
    group_width = QUERY_HEADS_HALF * HEAD_WIDTH // N_FRAME
    summed = jnp.zeros((sequence_length, MODEL_WIDTH), jnp.float32)
    for head_group in range(N_FRAME):
        columns = context[:, head_group * group_width:(head_group + 1) * group_width]
        partial_sum = jnp.dot(columns, wo[head_group * group_width:(head_group + 1) * group_width], preferred_element_type=jnp.float32)
        rounded = lax.optimization_barrier(partial_sum.astype(jnp.bfloat16))
        summed = summed + rounded.astype(jnp.float32)
    return summed.astype(jnp.bfloat16).reshape(TOK_OWN, DEVICES, MODEL_WIDTH)
```

```python
import math

import jax
import jax.numpy as jnp
from jax import lax
from jax.experimental import pallas as pl
from jax.experimental.pallas import tpu as pltpu
from jax.sharding import PartitionSpec as P

VHEADS = 16
HEAD_WIDTH = 128


rope_theta = 500000.0
vit_epsilon = 1e-06
norm_epsilon = 1e-05
masked_score = -1e30


def partner_2(value, axis, stride):
    mask = 2**stride
    pairs = [(source, source ^ mask) for source in range(lax.axis_size(axis))]
    return lax.ppermute(value, axis, pairs)


T_TILE = 16


def attend_kernel(seq_ref, q_ref, kv_ref, out_ref):
    tile = pl.program_id(0)
    my_seq = seq_ref[0]
    slots = q_ref.shape[0]
    groups = kv_ref.shape[0]
    rows = slots * T_TILE
    wide = q_ref[...].reshape(rows, 2 * HEAD_WIDTH)
    q = jnp.concatenate([wide[:, :HEAD_WIDTH], wide[:, HEAD_WIDTH:]], axis=0)
    keys_n = groups * T_TILE
    chunk = 1024
    state = (
        jnp.full((2 * rows, 1), masked_score, jnp.float32),
        jnp.zeros((2 * rows, 2 * HEAD_WIDTH), jnp.float32),
    )
    ones = jnp.ones((chunk, HEAD_WIDTH), jnp.bfloat16)

    def block(j, state, diagonal):
        kv = kv_ref[:, pl.ds(pl.multiple_of(j * T_TILE, T_TILE), T_TILE), :].reshape(
            keys_n, 2 * HEAD_WIDTH
        )
        scores = []
        for c in range(keys_n // chunk):
            part = kv[c * chunk : (c + 1) * chunk, :HEAD_WIDTH]
            scores.append(
                lax.dot_general(
                    q, part, (((1,), (1,)), ((), ())), preferred_element_type=jnp.float32
                )
            )
        high, acc = state
        for c in range(keys_n // chunk):
            score = scores[c]
            if diagonal:
                row = lax.broadcasted_iota(jnp.int32, (2 * rows, 1), 0) % rows
                row_pos = row % T_TILE * 128 + row // T_TILE * 16 + my_seq
                col = lax.broadcasted_iota(jnp.int32, (1, chunk), 1) + c * chunk
                group = col // T_TILE
                col_pos = col % T_TILE * 128 + group % slots * 16 + group // slots
                score = jnp.where(col_pos <= row_pos, score, masked_score)
            new_high = jnp.maximum(high, jnp.max(score, axis=1, keepdims=True))
            e = jnp.exp2(score - new_high).astype(jnp.bfloat16)
            values = jnp.concatenate([kv[c * chunk : (c + 1) * chunk, HEAD_WIDTH:], ones], axis=1)
            acc = acc * jnp.exp2(high - new_high) + jnp.dot(
                e, values, preferred_element_type=jnp.float32
            )
            high = new_high
        return (high, acc)

    state = block(tile, state, True)
    state = lax.fori_loop(0, tile, lambda j, st: block(j, st, False), state)
    acc = state[1]
    context = (acc[:, :HEAD_WIDTH] / acc[:, HEAD_WIDTH:]).astype(jnp.bfloat16)
    context = jnp.concatenate([context[:rows], context[rows:]], axis=1)
    out_ref[...] = context.reshape(slots, T_TILE, 2 * HEAD_WIDTH)


def attend(my_seq, q, kv):
    slots, frames, width = q.shape
    return pl.pallas_call(
        attend_kernel,
        grid=(frames // T_TILE,),
        in_specs=[
            pl.BlockSpec(memory_space=pltpu.SMEM),
            pl.BlockSpec((slots, T_TILE, width), lambda i: (0, i, 0)),
            pl.BlockSpec(memory_space=pltpu.VMEM),
        ],
        out_specs=pl.BlockSpec((slots, T_TILE, width), lambda i: (0, i, 0)),
        out_shape=jax.ShapeDtypeStruct((slots, frames, width), jnp.bfloat16),
        name="attend",
    )(my_seq, q, kv)


def apply_rotary(values, rotary_angles):
    half_width = values.shape[-1] // 2
    first_half = values[..., :half_width]
    second_half = values[..., half_width:]
    cosine = jnp.cos(rotary_angles)
    sine_part = jnp.sin(rotary_angles)
    return jnp.concatenate(
        [
            first_half * cosine - second_half * sine_part,
            second_half * cosine + first_half * sine_part,
        ],
        axis=-1,
    )


def rope_angles(positions, head_size):
    exponents = jnp.arange(0, head_size, 2).astype(jnp.float32) / head_size
    inverse = jnp.power(jnp.float32(rope_theta), -exponents)
    return positions.astype(jnp.float32)[:, None] * inverse[None, :]


def add_columns(left, shard_piece):
    return jnp.dot(left, shard_piece, preferred_element_type=jnp.float32)


def per_device(
    vit_states,
    frame_slot,
    patch_count,
    vis_start,
    text_embed,
    vit_ln_gain,
    vit_ln_bias,
    vit_qkv_w,
    vit_qkv_b,
    vit_out_w,
    vit_out_b,
    proj_w,
    proj_b,
    attn_gain,
    wq,
    wk,
    wv,
    wo,
):
    frames_n = lax.axis_size("frame")
    seqs_n = lax.axis_size("seq")
    devices_n = frames_n * seqs_n
    my_frame = lax.axis_index("frame")
    my_seq = lax.axis_index("seq")
    my_device = my_frame * seqs_n + my_seq
    slots_held = vit_states.shape[0]
    frame_max = vit_states.shape[1]
    width_vit = vit_states.shape[2]
    vis_max = frame_max // 4
    own_rows = text_embed.shape[0]
    laps = (vis_max + devices_n - 1) // devices_n
    frame_ids = jnp.arange(frame_slot.shape[0])
    holder = frame_slot // slots_held
    holder_frame = holder // seqs_n
    pair_low = (holder_frame - holder_frame % 2) * seqs_n + holder % seqs_n
    pair_order = holder_frame % 2 * slots_held + frame_slot % slots_held
    same_pair = pair_low[:, None] == pair_low[None, :]
    earlier = pair_order[None, :] < pair_order[:, None]
    pair_rank = jnp.sum((same_pair & earlier).astype(jnp.int32), axis=1)
    partner = partner_2(vit_states, "frame", 0)
    low_side = my_frame % 2 == 0
    four_slots = jnp.where(
        low_side,
        jnp.concatenate([vit_states, partner], 0),
        jnp.concatenate([partner, vit_states], 0),
    )
    my_low = (my_frame - my_frame % 2) * seqs_n + my_seq
    picked = (pair_low == my_low) & (pair_rank == my_frame % 2)
    my_frame_id = jnp.sum(jnp.where(picked, frame_ids, 0))
    my_order = jnp.sum(jnp.where(picked, pair_order, 0))
    states = lax.dynamic_slice_in_dim(four_slots, my_order, 1, 0)
    slots_n = 1
    slot_frames = jnp.reshape(my_frame_id, (1,))
    slot_live = jnp.ones((1,), jnp.bool_)
    source_device = pair_low + pair_rank * seqs_n
    slot_count = jnp.where(slot_live, patch_count[slot_frames], frame_max)
    slot_start = vis_start[slot_frames]
    patch_rows = states.reshape(slots_n * frame_max, width_vit)
    rows_wide = patch_rows.astype(jnp.float32)
    average = jnp.mean(rows_wide, axis=1, keepdims=True)
    centred = rows_wide - average
    spread = jnp.mean(centred * centred, axis=1, keepdims=True)
    normed_states = (centred * lax.rsqrt(spread + vit_epsilon) * vit_ln_gain + vit_ln_bias).astype(
        jnp.bfloat16
    )
    projected_vit = add_columns(normed_states, lax.all_gather(vit_qkv_w, "seq", axis=0, tiled=True))
    projected_vit = (projected_vit + vit_qkv_b).astype(jnp.bfloat16)
    head_size = width_vit // VHEADS
    shaped = projected_vit.reshape(slots_n, frame_max, 3, VHEADS, head_size)
    scores = jnp.einsum(
        "sqhd,skhd->shqk", shaped[:, :, 0], shaped[:, :, 1], preferred_element_type=jnp.float32
    ) / math.sqrt(head_size)
    key_live = jnp.arange(frame_max)[None, :] < slot_count[:, None]
    scores = jnp.where(key_live[:, None, None, :], scores, masked_score)
    highest = jnp.max(scores, axis=-1, keepdims=True)
    weights = jnp.exp(scores - highest)
    probabilities = (weights / jnp.sum(weights, axis=-1, keepdims=True)).astype(jnp.bfloat16)
    context_vit = jnp.einsum(
        "shqk,skhd->sqhd", probabilities, shaped[:, :, 2], preferred_element_type=jnp.float32
    ).astype(jnp.bfloat16)
    context_vit = context_vit.reshape(patch_rows.shape[0], width_vit)
    attended = add_columns(context_vit, lax.all_gather(vit_out_w, "seq", axis=0, tiled=True))
    hidden = (rows_wide + attended + vit_out_b).astype(jnp.bfloat16)
    pooled = jnp.mean(
        hidden.astype(jnp.float32).reshape(slots_n, vis_max, 4, width_vit), axis=2
    ).astype(jnp.bfloat16)
    owners = jnp.arange(devices_n)
    lap_ids = jnp.arange(laps)
    distance = jnp.mod(owners[:, None] - slot_start[None, :], devices_n)
    token_ids = distance[:, :, None] + lap_ids[None, None, :] * devices_n
    sent_live = (token_ids < (slot_count // 4)[None, :, None]) & slot_live[None, :, None]
    token_clip = jnp.minimum(token_ids, vis_max - 1)
    slot_ids = jnp.arange(slots_n)[None, :, None]
    outgoing = jnp.where(
        sent_live[..., None], pooled[slot_ids, token_clip], jnp.zeros((), jnp.bfloat16)
    )
    arrived = lax.all_to_all(outgoing, ("frame", "seq"), split_axis=0, concat_axis=0, tiled=True)
    local_ids = jnp.arange(own_rows)
    positions = local_ids * devices_n + my_device
    token_frame = positions // own_rows
    within = positions - vis_start[token_frame]
    is_visual = (within >= 0) & (within < patch_count[token_frame] // 4)
    within_clip = jnp.clip(within, 0, vis_max - 1)
    flat_index = source_device[token_frame] * slots_n * laps + within_clip // devices_n
    table = arrived.reshape(devices_n * slots_n * laps, arrived.shape[-1])
    fetched = table[flat_index]
    fetched = (jnp.dot(fetched, proj_w, preferred_element_type=jnp.float32) + proj_b).astype(
        jnp.bfloat16
    )
    text_rows = text_embed.reshape(own_rows, text_embed.shape[-1])
    merged = jnp.where(is_visual[:, None], fetched, text_rows)
    merged_wide = merged.astype(jnp.float32)
    normed_tok = (
        merged_wide
        * lax.rsqrt(jnp.mean(merged_wide * merged_wide, axis=1, keepdims=True) + norm_epsilon)
        * attn_gain
    ).astype(jnp.bfloat16)
    shard_piece = lax.all_gather(normed_tok, "frame", axis=0, tiled=True)
    projected = jnp.concatenate(
        [
            jnp.dot(shard_piece, wq, preferred_element_type=jnp.float32),
            jnp.dot(shard_piece, wk, preferred_element_type=jnp.float32),
            jnp.dot(shard_piece, wv, preferred_element_type=jnp.float32),
        ],
        axis=1,
    )
    query_width = wq.shape[1]
    kv_width = wk.shape[1]
    group_rows = projected.shape[0]
    kv_heads = kv_width // HEAD_WIDTH
    query_heads = query_width // HEAD_WIDTH
    row_ids = jnp.arange(group_rows)
    group_positions = row_ids % own_rows * devices_n + row_ids // own_rows * seqs_n + my_seq
    rotary_angles = rope_angles(group_positions, HEAD_WIDTH)[:, None, :]
    query_matrix = (
        apply_rotary(
            projected[:, :query_width].reshape(group_rows, query_heads, HEAD_WIDTH), rotary_angles
        )
        * (math.log2(math.e) / math.sqrt(HEAD_WIDTH))
    ).astype(jnp.bfloat16)
    keys_own = apply_rotary(
        projected[:, query_width : query_width + kv_width].reshape(
            group_rows, kv_heads, HEAD_WIDTH
        ),
        rotary_angles,
    ).astype(jnp.bfloat16)
    values_own = (
        projected[:, query_width + kv_width :]
        .astype(jnp.bfloat16)
        .reshape(group_rows, kv_heads, HEAD_WIDTH)
    )
    kv_own = jnp.concatenate(
        [keys_own.reshape(group_rows, kv_width), values_own.reshape(group_rows, kv_width)], axis=1
    )
    kv_all = lax.all_gather(kv_own, "seq", axis=0, tiled=True).reshape(
        seqs_n * frames_n, own_rows, 2 * kv_width
    )
    context_tok = attend(
        my_seq.reshape(1).astype(jnp.int32),
        query_matrix.reshape(frames_n, own_rows, query_width),
        kv_all,
    ).reshape(group_rows, query_width)
    summed = lax.psum_scatter(
        jnp.dot(context_tok, wo, preferred_element_type=jnp.float32).astype(jnp.bfloat16),
        "frame",
        scatter_dimension=0,
        tiled=True,
    )
    return summed.reshape(own_rows, 1, wo.shape[1])


def solution(mesh):
    return jax.shard_map(
        per_device,
        mesh=mesh,
        in_specs=(
            P(("frame", "seq"), None, None),
            P(),
            P(),
            P(),
            P(None, ("frame", "seq"), None),
            P(),
            P(),
            P("seq", None),
            P(),
            P("seq", None),
            P(),
            P(),
            P(),
            P(),
            P(None, "frame"),
            P(None, "frame"),
            P(None, "frame"),
            P("frame", None),
        ),
        out_specs=P(None, ("frame", "seq"), None),
        check_vma=False,
    )
```
